32 devices in a mesh: unit: 4 (over z), bank: 4 (over x, core), zero: 2 (over y).
Axes of the slice: x: 2, y: 2, z: 4, core: 2. Of those that a mesh axis runs over, the one named last changes fastest.
Arguments:
- train_down: float32 [256, 1024, 2048], P(('unit', 'bank'), None, 'zero'), parts along dimension 0, may hold values from -0.25 to 0.25
- router_weight: float32 [8192, 64], P(('unit', 'zero'), 'bank'), parts along dimension 0, may hold values from -0.125 to 0.125
- router_gain: float32 [8192], P(('unit', 'zero')), parts along dimension 0, may hold values from 0.25 to 1.75
Outputs:
- ready_down: bfloat16 [256, 1024, 2048], P(('unit', 'bank'), 'zero'), parts along dimension 0
- scale_down: float32 [256, 1024], P(('unit', 'bank'), 'zero'), parts along dimension 0
- serve_router: bfloat16 [8192, 64], P('unit'), parts along dimension 0
The draws below stay inside these ranges and needn't reach their ends.
There are 4 independent parts, one for each index of `unit`. The reference program is written for one: setup_inputs(seed, part) draws one part's arguments, and reference() takes and returns one part's arrays. A program takes and returns all parts, laid end to end along the dimension named above; each array names one. Nothing has to cross between parts.
All inputs are finite; a program needn't handle non-finite values.
Results may differ from the reference program's by a relative error of at most 0.001.
Values may be sent and summed in bfloat16 or wider, within the bound.
A program may use at most 256 MiB of HBM per device.

```python
import jax
import jax.numpy as jnp

EXPERTS = 64
D_MODEL = 2048
D_EXPERT = 1024


def with_spikes(drawn, own_key, source, target, parts, factor):
    owner, partner = [(jnp.arange(drawn.shape[axis_at]) // (drawn.shape[axis_at] // parts)).reshape([-1 if axis == axis_at else 1 for axis in range(drawn.ndim)]) for axis_at in (source, target)]
    chosen = jax.random.permutation(own_key, parts)[partner]
    strong = (owner == chosen) | (owner == (partner + parts // 2) % parts)
    return jnp.where(strong, factor * drawn, drawn)


def levels(rng, extent, split, smallest, high):
    gain = 1.0
    for position, shards_of in split:
        draws = jax.random.uniform(jax.random.fold_in(jax.random.fold_in(rng, 6), position), (shards_of,), jnp.float32, smallest / len(split), high / len(split))
        gain = gain * jnp.repeat(jnp.exp(draws), extent[position] // shards_of).reshape((-1,) + (1,) * (len(extent) - 1 - position))
    return gain


def gaussian(own_key, dims, spread, most, shards=(), dtype=jnp.bfloat16):
    array = jax.random.normal(own_key, dims, jnp.float32) * spread
    if len(shards) > 0:
        array = levels(own_key, dims, shards, -0.22, 0.18) * array
    return jnp.clip(array, min=-most, max=most).astype(dtype)


def bell_draw_with(stream_key, extent, width, bound, pieces, heavy, held_as=jnp.bfloat16):
    entries = width * jax.random.normal(stream_key, extent, jnp.float32)
    if pieces:
        entries = entries * levels(stream_key, extent, pieces, -0.22, 0.18)
    return jnp.clip(with_spikes(entries, jax.random.fold_in(stream_key, 3), *heavy), -bound, bound).astype(held_as)


def setup_inputs(seed: int = 0, part: int = 0) -> dict:
    seeds = jax.random.split(jax.random.key(seed), 4)
    part_keys = jax.random.split(jax.random.fold_in(seeds[3], part), 4)
    return {
        "train_down": bell_draw_with(part_keys[0], (EXPERTS, D_EXPERT, D_MODEL), D_EXPERT ** -0.5, 0.25, ((0, 4), (2, 2)), (2, 1, 2, 2.0), jnp.float32),
        "router_weight": gaussian(part_keys[1], (D_MODEL, EXPERTS), D_MODEL ** -0.5, 0.125, ((0, 2), (1, 4)), jnp.float32),
        "router_gain": jnp.clip(1.0 + 0.15 * jax.random.normal(part_keys[2], (D_MODEL,), jnp.float32), 0.25, 1.75),
    }


def reference(train_down, router_weight, router_gain):
    scale_down = jnp.max(jnp.abs(train_down), axis=2)
    ready_down = (train_down / jnp.expand_dims(scale_down, 2)).astype(jnp.bfloat16)
    serve_router = (router_weight * router_gain[:, None]).astype(jnp.bfloat16)
    return ready_down, scale_down, serve_router
```

```python
import jax
import jax.numpy as jnp
from jax import lax
from jax.experimental import pallas as pl
from jax.experimental.pallas import tpu as pltpu
from jax.sharding import PartitionSpec as P


def place_kernel(column_ref, piece_ref, *refs):
    refs[-1][...] = piece_ref[...]


def place(piece, column, first, shape, ready=None):
    experts, rows, columns = piece.shape
    in_specs = [pl.BlockSpec((1, rows, columns), lambda i, at: (i, 0, 0))]
    operands = [column, piece]
    aliases = {}
    if ready is not None:
        in_specs.append(pl.BlockSpec(memory_space=pl.ANY))
        operands.append(ready)
        aliases = {2: 0}
    return pl.pallas_call(
        place_kernel,
        out_shape=jax.ShapeDtypeStruct(shape, piece.dtype),
        grid_spec=pltpu.PrefetchScalarGridSpec(
            num_scalar_prefetch=1,
            grid=(experts,),
            in_specs=in_specs,
            out_specs=pl.BlockSpec((1, rows, columns), lambda i, at: (first + i, 0, at[0])),
        ),
        input_output_aliases=aliases,
        cost_estimate=pl.CostEstimate(
            flops=0, bytes_accessed=2 * piece.size * piece.dtype.itemsize, transcendentals=0
        ),
        name="place",
    )(*operands)


def chunks_of(experts, n):
    if n > 2 or experts < 8:
        return [experts]
    middle = experts - 5
    return [1, 1, 1] + [2] * (middle // 2) + [1] * (middle % 2) + [1, 1]


def per_device(train_down, router_weight, router_gain):
    n = lax.axis_size("zero")
    me = lax.axis_index("zero")
    experts, all_rows, columns = train_down.shape
    rows = all_rows // n
    shape = (experts, rows, n * columns)

    def shift(value, step):
        return lax.ppermute(value, "zero", [(i, (i + step) % n) for i in range(n)])

    def to_step(step):
        return lax.rem(me + step, n)

    def after(value, first):
        return lax.optimization_barrier((value, first))

    def local_max(block):
        return jnp.max(jnp.abs(block), axis=2)

    def whole_max(part):
        whole = part
        for step in range(1, n):
            whole = jnp.maximum(whole, shift(part, step))
        return whole

    def narrow(source, first, size, scale, owner):
        block = lax.dynamic_slice(source, (first, owner * rows, 0), (size, rows, columns))
        by = lax.dynamic_slice(scale, (0, owner * rows), (size, rows))
        return (block / jnp.expand_dims(by, 2)).astype(jnp.bfloat16)

    sizes = chunks_of(experts, n)
    firsts = [sum(sizes[:k]) for k in range(len(sizes))]

    groups = [(0, 1), (1, 2), (3, experts - 3)] if len(sizes) > 1 else [(0, experts)]
    scales, arrived = [], []
    source = train_down

    def find_scale(source):
        at, span = groups[len(scales)]
        part = local_max(lax.slice_in_dim(source, at, at + span, axis=0))
        source, part = after(source, part)
        scales.append(whole_max(part))
        return source

    def scale_for(first, size):
        for g, (at, span) in enumerate(groups[: len(scales)]):
            if at <= first and first + size <= at + span:
                return lax.slice_in_dim(scales[g], first - at, first - at + size, axis=0)

    for _ in range(min(2, len(groups))):
        source = find_scale(source)
    for k, (first, size) in enumerate(zip(firsts, sizes)):
        for step in range(1, n):
            piece = narrow(source, first, size, scale_for(first, size), to_step(step))
            source, piece = after(source, piece)
            arrived.append((shift(piece, step), to_step(n - step), first))
        if k == 0:
            router_weight, piece = after(router_weight, piece)
            if len(scales) < len(groups):
                source = find_scale(source)
        if k == min(5, len(sizes) - 1):
            mark = piece

    scale = jnp.concatenate([scales[g] for g in range(len(groups))], axis=0)
    own = narrow(source, 0, experts, scale, me)
    ready_down = place(own, me[None], 0, shape)
    scale_down = lax.dynamic_slice_in_dim(scale, me * rows, rows, axis=1)

    part_router = (router_weight * router_gain[:, None]).astype(jnp.bfloat16).T
    depth = part_router.shape[1]
    row_router = jnp.zeros((part_router.shape[0], n * depth), jnp.bfloat16)
    row_router = lax.dynamic_update_slice(row_router, part_router, (0, me * depth))
    for step in range(1, n):
        piece = shift(part_router, step)
        row_router = lax.dynamic_update_slice(row_router, piece, (0, to_step(n - step) * depth))
    row_router, mark = after(row_router, mark)
    serve_router = lax.all_gather(row_router, "bank", axis=0, tiled=True).T

    ready_down, _ = after(ready_down, serve_router)
    for piece, source, first in arrived:
        ready_down = place(piece, source[None], first, shape, ready_down)
    return (ready_down, scale_down, serve_router)


def solution(mesh):
    in_specs = (P(("unit", "bank"), None, "zero"), P(("unit", "zero"), "bank"), P(("unit", "zero")))
    out_specs = (P(("unit", "bank"), "zero", None), P(("unit", "bank"), "zero"), P("unit", None))
    return jax.shard_map(
        per_device, mesh=mesh, in_specs=in_specs, out_specs=out_specs, check_vma=False
    )
```
